128 devices in a mesh: occ: 8 (over z, core), pan: 16 (over y, x).
Axes of the slice: x: 4, y: 4, z: 4, core: 2. Of those that a mesh axis runs over, the one named last changes fastest.
Arguments:
- gamma_ia: bfloat16 [2, 1024, 8704], P(None, 'occ', 'pan'), may hold values from -6 to 6
- coef_virt: bfloat16 [10240, 8704], P(None, 'pan'), may hold values from -0.09375 to 0.09375
- coef_occ: bfloat16 [10240, 1024], P('occ'), may hold values from -0.1875 to 0.1875
- tile_mask: int32 [80, 80], replicated, may hold values from 0 to 1, as said below
- tile_owner: int32 [80, 80], replicated, may hold values from 0 to 15, as said below
Outputs:
- gradient_tiles: bfloat16 [8, 16, 16, 2, 2, 128, 128], P('occ', 'pan')
The draws below stay inside these ranges and needn't reach their ends.
Inputs may be any that keep to these rules, and one draw needn't show every extreme that they name: `tile_mask`: each block of 10 x 5 tiles holds at most 32 ones. `tile_owner`: within each block of 10 x 5 tiles, at most 2 tiles with tile_mask 1 share an owner; in every draw some block gives exactly 2 such tiles to one owner.
All inputs are finite; a program needn't handle non-finite values.
Results may differ from the reference program's by a relative error of at most 0.005.
Values may be sent and summed in bfloat16 or wider, within the bound.
No kernel may reach another device: no remote copies, remote signals or barrier semaphores. Data moves between devices by JAX's collectives and lax.ppermute only.
A program may use at most 128 MiB of HBM per device.

```python
import jax
import jax.numpy as jnp
from jax import lax

NOCC = 1024
NVIR = 8704
NAO = 10240
AUX = 2
TILE = 128
SCAP = 2
NT = 80
MT = 10
NTP = 5
OWNERS = 16
N_OCC = 8
N_PAN = 16


def tile_pattern(key):
    base = jax.random.fold_in(key, 913)
    first = jax.random.fold_in(base, 1)
    second = jax.random.fold_in(base, 2)
    third = jax.random.fold_in(base, 3)
    fourth = jax.random.fold_in(base, 4)
    row_index = lax.broadcasted_iota(jnp.int32, (NT, NT), 0)
    col_index = lax.broadcasted_iota(jnp.int32, (NT, NT), 1)
    spacing = jnp.abs(row_index - col_index)
    limit = jnp.maximum(150, 850 - 25 * spacing)
    screened = (jax.random.randint(first, (NT, NT), 0, 1000) < limit) | (row_index < MT) & (col_index < NTP)
    scores = jax.random.randint(second, (NT, NT), 0, 4096) * (NT * NT) + row_index * NT + col_index
    ordered = jnp.where(screened, scores, scores + 4096 * NT * NT)
    row_blocks = NT // MT
    col_blocks = NT // NTP
    blocked = ordered.reshape(row_blocks, MT, col_blocks, NTP).transpose(0, 2, 1, 3).reshape(row_blocks, col_blocks, MT * NTP)
    places = jnp.argsort(jnp.argsort(blocked, axis=-1), axis=-1).astype(jnp.int32)
    places = places.reshape(row_blocks, col_blocks, MT, NTP).transpose(0, 2, 1, 3).reshape(NT, NT)
    kept = screened & (places < OWNERS * SCAP)
    turns = jax.random.randint(third, (row_blocks, col_blocks), 0, OWNERS)
    turns = jnp.repeat(jnp.repeat(turns, MT, axis=0), NTP, axis=1)
    stray = jax.random.randint(fourth, (NT, NT), 0, OWNERS)
    owners_of = jnp.where(kept, (places + turns) % OWNERS, stray).astype(jnp.int32)
    return (kept.astype(jnp.int32), owners_of)


def draw_tile_mask(key, part):
    return tile_pattern(key)[0]


def draw_tile_owner(key, part):
    return tile_pattern(key)[1]


def strengthened(array, stream_key, source, target, parts, factor):
    def block_of(axis_at):
        return (jnp.arange(array.shape[axis_at]) // (array.shape[axis_at] // parts)).reshape((-1,) + (1,) * (array.ndim - 1 - axis_at))

    first = jax.random.permutation(stream_key, parts)[block_of(target)]
    other_side = (block_of(target) + parts // 2) % parts
    return jnp.where((block_of(source) == first) | (block_of(source) == other_side), factor * array, array)


def steps_of(key, dims, shards, smallest, largest):
    loudness = 1.0
    for axis_at, shards_of in shards:
        steps = jax.random.uniform(jax.random.fold_in(jax.random.fold_in(key, 6), axis_at), (shards_of,), jnp.float32, smallest / len(shards), largest / len(shards))
        loudness = loudness * jnp.repeat(jnp.exp(steps), dims[axis_at] // shards_of).reshape((-1,) + (1,) * (len(dims) - 1 - axis_at))
    return loudness


def scatter_about(own_key, extent, spread, reach, split=(), held_as=jnp.bfloat16):
    gain = steps_of(own_key, extent, split, -0.22, 0.18) if split else 1.0
    drawn = jax.random.normal(own_key, extent, jnp.float32) * spread * gain
    return jnp.minimum(jnp.maximum(drawn, -reach), reach).astype(held_as)


def gaussian_with(key, extent, scale, bound, shards, heavy, held_as=jnp.bfloat16):
    result = scale * jax.random.normal(key, extent, jnp.float32)
    if shards:
        result = result * steps_of(key, extent, shards, -0.22, 0.18)
    return jnp.clip(strengthened(result, jax.random.fold_in(key, 3), *heavy), -bound, bound).astype(held_as)


def setup_inputs(seed: int = 0) -> dict:
    arg_keys = jax.random.split(jax.random.key(seed), 6)
    gamma_ia = scatter_about(arg_keys[0], (AUX, NOCC, NVIR), 1.0, 6.0, ((1, 8), (2, 16)))
    coef_virt = gaussian_with(arg_keys[1], (NAO, NVIR), NVIR ** -0.5, 0.09375, ((1, 16),), (1, 0, 16, 2.0))
    coef_occ = scatter_about(arg_keys[2], (NAO, NOCC), NOCC ** -0.5, 0.1875, ((0, 8),))
    tile_mask = draw_tile_mask(jax.random.fold_in(arg_keys[5], 71), 0)
    tile_owner = draw_tile_owner(jax.random.fold_in(arg_keys[5], 71), 0)
    return {"gamma_ia": gamma_ia, "coef_virt": coef_virt, "coef_occ": coef_occ, "tile_mask": tile_mask, "tile_owner": tile_owner}


def route_slots(block_mask, block_owner, owners):
    usable = block_mask.reshape(-1)
    owners_of = block_owner.reshape(-1)
    belongs = ((usable[:, None] == 1) & (owners_of[:, None] == jnp.arange(owners, dtype=jnp.int32)[None, :])).astype(jnp.int32)
    order_rank = jnp.cumsum(belongs, axis=0) - belongs
    matched = belongs[:, :, None] * (order_rank[:, :, None] == jnp.arange(SCAP, dtype=jnp.int32)[None, None, :]).astype(jnp.int32)
    tile_index = jnp.arange(usable.shape[0], dtype=jnp.int32)
    slot_tile = jnp.sum(matched * tile_index[:, None, None], axis=0).astype(jnp.int32)
    filled = jnp.sum(matched, axis=0)
    return slot_tile, filled


def reference(gamma_ia, coef_virt, coef_occ, tile_mask, tile_owner):
    gamma_flat = gamma_ia.reshape(AUX * NOCC, NVIR)
    half_x = lax.dot_general(gamma_flat, coef_virt, (((1,), (1,)), ((), ())), preferred_element_type=jnp.float32)
    half_x = half_x.astype(jnp.bfloat16).reshape(AUX, NOCC, NAO)

    def one_block(block_id):
        row_block = block_id // N_PAN
        col_block = block_id % N_PAN
        row_coef = lax.dynamic_slice(coef_occ, ((row_block * MT * TILE).astype(jnp.int32), jnp.int32(0)), (MT * TILE, NOCC))
        col_half = lax.dynamic_slice(half_x, (jnp.int32(0), jnp.int32(0), (col_block * NTP * TILE).astype(jnp.int32)), (AUX, NOCC, NTP * TILE))
        products = jnp.einsum("ri,pik->prk", row_coef.astype(jnp.float32), col_half.astype(jnp.float32))
        tile_set = products.reshape(AUX, MT, TILE, NTP, TILE).transpose(1, 3, 0, 2, 4).reshape(MT * NTP, AUX, TILE, TILE)
        block_mask = lax.dynamic_slice(tile_mask, ((row_block * MT).astype(jnp.int32), (col_block * NTP).astype(jnp.int32)), (MT, NTP))
        block_owner = lax.dynamic_slice(tile_owner, ((row_block * MT).astype(jnp.int32), (col_block * NTP).astype(jnp.int32)), (MT, NTP))
        slot_tile, filled = route_slots(block_mask, block_owner, N_PAN)
        picked = jnp.take(tile_set, slot_tile.reshape(-1), axis=0).reshape(N_PAN, SCAP, AUX, TILE, TILE)
        return (picked * filled.astype(jnp.float32)[:, :, None, None, None]).astype(jnp.bfloat16)

    every = lax.map(one_block, jnp.arange(N_OCC * N_PAN, dtype=jnp.int32))
    every = every.reshape(N_OCC, N_PAN, N_PAN, SCAP, AUX, TILE, TILE)
    return every.transpose(0, 2, 1, 3, 4, 5, 6)
```

```python
import functools

import jax
import jax.numpy as jnp
from jax import lax
from jax.experimental import pallas as pl
from jax.experimental.pallas import tpu as pltpu
from jax.sharding import PartitionSpec as P

AUX = 2
TILE = 128
SCAP = 2
SIDE = 4
CORES = 2
AXES = ("occ", "pan")


def device_id(z, c, y, x):
    return (z * CORES + c) * SIDE * SIDE + y * SIDE + x


def shifts(first=0, second=0, dz=0, swap=False):
    pairs = []
    for z in range(SIDE):
        for c in range(CORES):
            dy, dx = (second, first) if c == 0 else (first, second)
            for y in range(SIDE):
                for x in range(SIDE):
                    to = device_id((z + dz) % SIDE, c ^ int(swap), (y + dy) % SIDE, (x + dx) % SIDE)
                    pairs.append((device_id(z, c, y, x), to))
    return pairs


def send(value, **where):
    return lax.ppermute(value, AXES, shifts(**where))


def route_slots(block_mask, block_owner, owners):
    usable = block_mask.reshape(-1)
    owners_of = block_owner.reshape(-1)
    belongs = (
        (usable[:, None] == 1)
        & (owners_of[:, None] == jnp.arange(owners, dtype=jnp.int32)[None, :])
    ).astype(jnp.int32)
    order_rank = jnp.cumsum(belongs, axis=0) - belongs
    matched = belongs[:, :, None] * (
        order_rank[:, :, None] == jnp.arange(SCAP, dtype=jnp.int32)[None, None, :]
    ).astype(jnp.int32)
    tile_index = jnp.arange(usable.shape[0], dtype=jnp.int32)
    slot_tile = jnp.sum(matched * tile_index[:, None, None], axis=0)
    filled = jnp.sum(matched, axis=0)
    return (slot_tile, filled)


def partial_kernel(panel, coef_ref, gamma_ref, *outs):
    width = gamma_ref.shape[0] // AUX
    part = lax.dot_general(
        coef_ref[...], gamma_ref[...], (((1,), (1,)), ((), ())), preferred_element_type=jnp.float32
    )
    for p in range(AUX):
        outs[p][0] = part[:, p * width : (p + 1) * width].astype(outs[p].dtype)


def partial_sums(panel, coef_virt, gamma, first, dtype):
    rows = coef_virt.shape[0] // (SIDE * SIDE)
    depth = coef_virt.shape[1]
    width = gamma.shape[0] // AUX
    out = jax.ShapeDtypeStruct((SIDE, rows, width), dtype)
    return pl.pallas_call(
        partial_kernel,
        grid_spec=pltpu.PrefetchScalarGridSpec(
            num_scalar_prefetch=1,
            grid=(SIDE,),
            in_specs=[
                pl.BlockSpec((rows, depth), lambda e, panel: (panel[first * SIDE + e], 0)),
                pl.BlockSpec(gamma.shape, lambda e, panel: (0, 0)),
            ],
            out_specs=[pl.BlockSpec((1, rows, width), lambda e, panel: (e, 0, 0))] * AUX,
        ),
        out_shape=[out] * AUX,
        name=f"partial_{first}",
    )(panel, coef_virt, gamma)


def dense_kernel(place, coef_ref, *refs):
    blocks = refs[: SIDE * CORES]
    outs = refs[SIDE * CORES : SIDE * CORES + SIDE]
    whole, dense = refs[SIDE * CORES + SIDE :]
    slots = SIDE * SIDE * SCAP
    for k, block in enumerate(blocks):
        at = pl.multiple_of(place[3 * slots + k] * TILE, TILE)
        whole[pl.ds(at, TILE), :] = block[...]
    dense[...] = jnp.dot(coef_ref[...], whole[...], preferred_element_type=jnp.float32).astype(dense.dtype)
    for d in range(SIDE):
        for e in range(SIDE):
            for k in range(SCAP):
                n = (d * SIDE + e) * SCAP + k
                row = pl.multiple_of(place[n] * TILE, TILE)
                column = pl.multiple_of(place[slots + n] * TILE, TILE)
                tile = dense[pl.ds(row, TILE), pl.ds(column, TILE)]
                outs[d][e, k] = jnp.where(place[2 * slots + n] == 1, tile, jnp.zeros_like(tile))


def picked_tiles(place, coef_occ, blocks):
    rows, depth = coef_occ.shape
    columns = blocks[0].shape[1]
    out = jax.ShapeDtypeStruct((SIDE, SCAP, TILE, TILE), jnp.bfloat16)
    vmem = pl.BlockSpec(memory_space=pltpu.VMEM)
    return pl.pallas_call(
        dense_kernel,
        in_specs=[pl.BlockSpec(memory_space=pltpu.SMEM)] + [vmem] * (1 + len(blocks)),
        out_specs=[vmem] * SIDE,
        out_shape=[out] * SIDE,
        scratch_shapes=[
            pltpu.VMEM((depth, columns), jnp.bfloat16),
            pltpu.VMEM((rows, columns), jnp.bfloat16),
        ],
        name="dense",
    )(place, coef_occ, *blocks)


def place_kernel(source, *refs):
    out = refs[-1]
    step = pl.program_id(0)
    for e in range(SIDE):

        @pl.when(step // SIDE == e)
        def _():
            for p in range(AUX):
                out[0, 0, 0, :, p] = refs[p * SIDE + e][0]


def assembled(source, received):
    def block_at(e):
        return lambda step, source: (
            jnp.clip(step - e * SIDE, 0, SIDE - 1),
            0,
            0,
            0,
        )

    return pl.pallas_call(
        place_kernel,
        grid_spec=pltpu.PrefetchScalarGridSpec(
            num_scalar_prefetch=1,
            grid=(SIDE * SIDE,),
            in_specs=[pl.BlockSpec((1, SCAP, TILE, TILE), block_at(e)) for p in range(AUX) for e in range(SIDE)],
            out_specs=pl.BlockSpec(
                (1, 1, 1, SCAP, AUX, TILE, TILE), lambda step, source: (0, 0, source[step], 0, 0, 0, 0)
            ),
        ),
        out_shape=jax.ShapeDtypeStruct((1, 1, SIDE * SIDE, SCAP, AUX, TILE, TILE), jnp.bfloat16),
        name="assemble",
    )(source, *[received[p][e] for p in range(AUX) for e in range(SIDE)])


def local(gamma_ia, coef_virt, coef_occ, tile_mask, tile_owner):
    panels = SIDE * SIDE
    row_tiles = coef_occ.shape[0] // TILE
    col_tiles = coef_virt.shape[0] // panels // TILE
    gamma = gamma_ia.reshape(AUX * gamma_ia.shape[1], gamma_ia.shape[2])
    row_block = lax.axis_index("occ")
    col_block = lax.axis_index("pan")
    depth_at, core = row_block // CORES, row_block % CORES
    high, low = col_block // SIDE, col_block % SIDE
    first_at = jnp.where(core == 0, low, high)
    second_at = jnp.where(core == 0, high, low)

    def panel_of(first, second):
        return jnp.where(core == 0, second * SIDE + first, first * SIDE + second)

    step = jnp.arange(panels, dtype=jnp.int32)
    panel = panel_of((first_at + step // SIDE) % SIDE, (second_at + step % SIDE) % SIDE)
    source = panel_of((first_at - step % SIDE) % SIDE, (second_at - step // SIDE) % SIDE)

    order = (2, 1, 3)
    parts = {}
    for d in order:
        parts[d] = partial_sums(panel, coef_virt, gamma, d, jnp.bfloat16)
    arrived = [{d: send(parts[d][p], first=d) for d in order} for p in range(AUX)]
    own = partial_sums(panel, coef_virt, gamma, 0, jnp.float32)

    block_mask = lax.dynamic_slice(
        tile_mask, (row_block * row_tiles, col_block * col_tiles), (row_tiles, col_tiles)
    )
    block_owner = lax.dynamic_slice(
        tile_owner, (row_block * row_tiles, col_block * col_tiles), (row_tiles, col_tiles)
    )
    slot_tile, filled = route_slots(block_mask, block_owner, panels)
    slot_tile = jnp.take(slot_tile, panel, axis=0).reshape(-1)
    filled = jnp.take(filled, panel, axis=0).reshape(-1)
    away = jnp.array([0, 1, 3, 2], dtype=jnp.int32)
    depths = (depth_at - away) % SIDE
    blocks_at = jnp.concatenate([depths * CORES + core, depths * CORES + 1 - core])
    place = jnp.concatenate([slot_tile // col_tiles, slot_tile % col_tiles, filled, blocks_at]).astype(jnp.int32)

    tiles = []
    for p in range(AUX):
        total = own[p]
        for d in order:
            total = total + arrived[p][d].astype(jnp.float32)
        here = {e: send(total[e].astype(jnp.bfloat16), second=e) for e in order}
        half = total[0]
        for e in order:
            half = half + here[e].astype(jnp.float32)
        half = half.T.astype(jnp.bfloat16)
        mine = [half] + [send(half, dz=dz) for dz in (1, 3, 2)]
        other = [send(block, swap=True) for block in mine]
        tiles.append(picked_tiles(place, coef_occ, mine + other))

    received = []
    for p in range(AUX):
        across = [tiles[p][0]] + [send(tiles[p][d], first=d) for d in range(1, SIDE)]
        gathered = [jnp.stack([across[d][e] for d in range(SIDE)]) for e in range(SIDE)]
        received.append([gathered[0]] + [send(gathered[e], second=e) for e in range(1, SIDE)])
    return assembled(source, received)


def solution(mesh):
    return jax.shard_map(
        local,
        mesh=mesh,
        in_specs=(P(None, "occ", "pan"), P(None, "pan"), P("occ", None), P(), P()),
        out_specs=P("occ", "pan", None, None, None, None, None),
        check_vma=False,
    )
```

```python
import functools

import jax
import jax.numpy as jnp
from jax import lax
from jax.experimental import pallas as pl
from jax.experimental.pallas import tpu as pltpu
from jax.sharding import PartitionSpec as P

AUX = 2
TILE = 128
SCAP = 2
SIDE = 4
CORES = 2
PANELS = SIDE * SIDE
SLOTS = PANELS * SCAP
AXES = ("occ", "pan")
MIB = 1 << 20
VMEM_SPEC = pl.BlockSpec(memory_space=pltpu.VMEM)
ANY_SPEC = pl.BlockSpec(memory_space=pl.ANY)
SMEM_SPEC = pl.BlockSpec(memory_space=pltpu.SMEM)


def device_id(z, c, y, x):
    return (z * CORES + c) * PANELS + y * SIDE + x


def shifts(first=0, second=0, dz=0, swap=False):
    pairs = []
    for z in range(SIDE):
        for c in range(CORES):
            dy, dx = (second, first) if c == 0 else (first, second)
            for y in range(SIDE):
                for x in range(SIDE):
                    to = device_id((z + dz) % SIDE, c ^ int(swap), (y + dy) % SIDE, (x + dx) % SIDE)
                    pairs.append((device_id(z, c, y, x), to))
    return pairs


def send(value, **where):
    return lax.ppermute(value, AXES, shifts(**where))


def here():
    row_block, panel = lax.axis_index("occ"), lax.axis_index("pan")
    z, core = lax.div(row_block, CORES), lax.rem(row_block, CORES)
    return z, core, lax.div(panel, SIDE), lax.rem(panel, SIDE)


def panel_at(first, second):
    _, core, y, x = here()
    dy = jnp.where(core == 0, second, first)
    dx = jnp.where(core == 0, first, second)
    return lax.rem(y + dy + SIDE, SIDE) * SIDE + lax.rem(x + dx + SIDE, SIDE)


def call(kernel, name, out_shape, operands, in_specs, out_specs, scratch=(), limit=8, flops=1000):
    return pl.pallas_call(
        kernel,
        in_specs=in_specs,
        out_specs=out_specs,
        out_shape=out_shape,
        scratch_shapes=scratch,
        compiler_params=pltpu.CompilerParams(vmem_limit_bytes=limit * MIB),
        cost_estimate=pl.CostEstimate(flops=flops, bytes_accessed=1000, transcendentals=0),
        name=name,
    )(*operands)


def near(value):
    return pltpu.with_memory_space_constraint(value, pltpu.VMEM)


def partial_kernel(first, coef_ref, gamma_ref, *refs):
    outs, (block, rows, sems) = refs[:AUX], refs[AUX:]
    width = block.shape[2]
    copies = []
    for e in range(SIDE):
        at = pl.multiple_of(panel_at(first, e) * width, TILE)
        copies.append(pltpu.make_async_copy(coef_ref.at[:, pl.ds(at, width)], block.at[e], sems.at[e]))
        copies[e].start()
    for p in range(AUX):
        rows[p * TILE : (p + 1) * TILE, :] = gamma_ref[p].T
    for e in range(SIDE):
        copies[e].wait()
        part = jnp.dot(rows[...], block[e], preferred_element_type=jnp.float32)
        for p in range(AUX):
            outs[p][e] = part[p * TILE : (p + 1) * TILE].astype(outs[p].dtype)


def partial_sums(coef, gamma, first, dtype):
    depth, columns = coef.shape
    width = columns // PANELS
    return call(
        functools.partial(partial_kernel, first),
        f"partial_{first}",
        [pltpu.VMEM((SIDE, TILE, width), dtype)] * AUX,
        (coef, gamma),
        [ANY_SPEC, VMEM_SPEC],
        [VMEM_SPEC] * AUX,
        scratch=[
            pltpu.VMEM((SIDE, depth, width), jnp.bfloat16),
            pltpu.VMEM((AUX * TILE, depth), jnp.bfloat16),
            pltpu.SemaphoreType.DMA((SIDE,)),
        ],
        limit=10,
    )


def total_kernel(own, a, b, c, zero, *outs):
    for e in range(SIDE):
        total = own[e] + a[e].astype(jnp.float32) + b[e].astype(jnp.float32) + c[e].astype(jnp.float32)
        if e == 0:
            zero[...] = total
        else:
            outs[e - 1][...] = total.astype(jnp.bfloat16)


def totals(own, arrived):
    shape = own.shape[1:]
    return call(
        total_kernel,
        "totals",
        [pltpu.VMEM(shape, jnp.float32)] + [pltpu.VMEM(shape, jnp.bfloat16)] * (SIDE - 1),
        (near(own), *[near(value) for value in arrived]),
        [VMEM_SPEC] * SIDE,
        [VMEM_SPEC] * SIDE,
    )


def half_kernel(own, a, b, c, out):
    out[...] = (
        own[...] + a[...].astype(jnp.float32) + b[...].astype(jnp.float32) + c[...].astype(jnp.float32)
    ).astype(out.dtype)


def half_of(own, arrived):
    return call(
        half_kernel,
        "half",
        pltpu.VMEM(own.shape, jnp.bfloat16),
        (near(own), *[near(value) for value in arrived]),
        [VMEM_SPEC] * SIDE,
        VMEM_SPEC,
    )


def route_kernel(row_tiles, col_tiles, mask, owner, place, count):
    row_at = lax.axis_index("occ") * row_tiles
    col_at = lax.axis_index("pan") * col_tiles
    for j in range(PANELS):
        count[j] = 0
    for n in range(3 * SLOTS):
        place[n] = 0
    for t in range(row_tiles):
        for u in range(col_tiles):
            kept = mask[row_at + t, col_at + u] == 1

            @pl.when(kept)
            def _():
                j = owner[row_at + t, col_at + u]
                k = jnp.minimum(count[j], SCAP - 1)
                count[j] = k + 1
                place[j * SCAP + k] = t
                place[SLOTS + j * SCAP + k] = u
                place[2 * SLOTS + j * SCAP + k] = 1


def routed(tile_mask, tile_owner, row_tiles, col_tiles):
    return call(
        functools.partial(route_kernel, row_tiles, col_tiles),
        "route",
        jax.ShapeDtypeStruct((3 * SLOTS,), jnp.int32),
        (tile_mask, tile_owner),
        [SMEM_SPEC] * 2,
        SMEM_SPEC,
        scratch=[pltpu.SMEM((PANELS,), jnp.int32)],
    )


AWAY = (0, 1, 3, 2)


def dense_kernel(place, coef_ref, *refs):
    blocks = refs[: SIDE * CORES]
    outs = refs[SIDE * CORES : SIDE * CORES + SIDE]
    whole, dense = refs[SIDE * CORES + SIDE :]
    z, core, _, _ = here()
    for n, block in enumerate(blocks):
        depth = lax.rem(z - AWAY[n % SIDE] + SIDE, SIDE)
        part = core if n < SIDE else 1 - core
        whole[pl.ds(pl.multiple_of((depth * CORES + part) * TILE, TILE), TILE), :] = block[...]
    dense[...] = jnp.dot(coef_ref[...], whole[...], preferred_element_type=jnp.float32).astype(dense.dtype)
    for d in range(SIDE):
        for e in range(SIDE):
            owner = panel_at(d, e)
            for k in range(SCAP):
                n = owner * SCAP + k
                row = pl.multiple_of(place[n] * TILE, TILE)
                column = pl.multiple_of(place[SLOTS + n] * TILE, TILE)
                tile = dense[pl.ds(row, TILE), pl.ds(column, TILE)]
                outs[d][e, k] = jnp.where(place[2 * SLOTS + n] == 1, tile, jnp.zeros_like(tile))


def picked_tiles(place, coef_occ, blocks):
    rows, depth = coef_occ.shape
    columns = blocks[0].shape[1]
    return call(
        dense_kernel,
        "dense",
        [pltpu.VMEM((SIDE, SCAP, TILE, TILE), jnp.bfloat16)] * SIDE,
        (place, near(coef_occ), *[near(block) for block in blocks]),
        [SMEM_SPEC] + [VMEM_SPEC] * (1 + len(blocks)),
        [VMEM_SPEC] * SIDE,
        scratch=[
            pltpu.VMEM((depth, columns), jnp.bfloat16),
            pltpu.VMEM((rows, columns), jnp.bfloat16),
        ],
        limit=16,
    )


def stack_kernel(*refs):
    across, outs = refs[:SIDE], refs[SIDE:]
    for e in range(SIDE):
        for d in range(SIDE):
            outs[e][d] = across[d][e]


def stacked(across):
    return call(
        stack_kernel,
        "stack",
        [pltpu.VMEM(across[0].shape, across[0].dtype)] * SIDE,
        [near(value) for value in across],
        [VMEM_SPEC] * SIDE,
        [VMEM_SPEC] * SIDE,
    )


def place_kernel(*refs):
    out, sems = refs[-2:]
    copies = []
    for p in range(AUX):
        for e in range(SIDE):
            for d in range(SIDE):
                source = panel_at(-d, -e)
                for k in range(SCAP):
                    copy = pltpu.make_async_copy(
                        refs[p * SIDE + e].at[d, k], out.at[0, 0, source, k, p], sems.at[len(copies)]
                    )
                    copy.start()
                    copies.append(copy)
    for copy in copies:
        copy.wait()


def assembled(received):
    operands = [near(received[p][e]) for p in range(AUX) for e in range(SIDE)]
    return call(
        place_kernel,
        "assemble",
        jax.ShapeDtypeStruct((1, 1, PANELS, SCAP, AUX, TILE, TILE), jnp.bfloat16),
        operands,
        [VMEM_SPEC] * len(operands),
        ANY_SPEC,
        scratch=[pltpu.SemaphoreType.DMA((AUX * SLOTS,))],
    )


def local(gamma_ia, coef_virt, coef_occ, tile_mask, tile_owner):
    row_tiles = coef_occ.shape[0] // TILE
    col_tiles = coef_virt.shape[0] // PANELS // TILE
    gamma = jnp.swapaxes(gamma_ia, 1, 2)
    coef = coef_virt.T
    order = (2, 1, 3)
    parts = {d: partial_sums(coef, gamma, d, jnp.bfloat16) for d in order}
    arrived = [[send(parts[d][p], first=d) for d in order] for p in range(AUX)]
    own = partial_sums(coef, gamma, 0, jnp.float32)
    place = routed(tile_mask, tile_owner, row_tiles, col_tiles)

    tiles = []
    for p in range(AUX):
        zero, *others = totals(own[p], arrived[p])
        half = half_of(zero, [send(others[e - 1], second=e) for e in order])
        mine = [half] + [send(half, dz=dz) for dz in AWAY[1:]]
        other = [send(block, swap=True) for block in mine]
        tiles.append(picked_tiles(place, coef_occ, mine + other))

    received = []
    for p in range(AUX):
        across = [tiles[p][0]] + [send(tiles[p][d], first=d) for d in range(1, SIDE)]
        gathered = stacked(across)
        received.append([gathered[0]] + [send(gathered[e], second=e) for e in range(1, SIDE)])
    return assembled(received)


def solution(mesh):
    return jax.shard_map(
        local,
        mesh=mesh,
        in_specs=(P(None, "occ", "pan"), P(None, "pan"), P("occ", None), P(), P()),
        out_specs=P("occ", "pan", None, None, None, None, None),
        check_vma=False,
    )
```
